32 devices in a mesh: row: 8 (over y, x, core), col: 4 (over z).
Axes of the slice: x: 2, y: 2, z: 4, core: 2. Of those that a mesh axis runs over, the one named last changes fastest.
Arguments:
- points: bfloat16 [4096, 128], P(('row', 'col')), may hold values from -6 to 6
- abar: bfloat16 [4096, 8, 4, 128], P('row', None, 'col'), may hold values from -6 to 6
- inv_scale: float32 [128], replicated, may hold values from 0.05 to 0.2
Outputs:
- point_grad: float32 [4096, 128], P(('row', 'col'))
The draws below stay inside these ranges and needn't reach their ends.
All inputs are finite; a program needn't handle non-finite values.
Results may differ from the reference program's by a relative error of at most 0.0052.
Values may be sent and summed in bfloat16 or wider, within the bound.
No kernel may reach another device: no remote copies, remote signals or barrier semaphores. Data moves between devices by JAX's collectives and lax.ppermute only.
A program may use at most 64 MiB of HBM per device.

```python
import math
import jax
import jax.numpy as jnp
from jax import lax

FEAT = 128
PTS = 128
NPTS = 4096
N_ROW = 8
N_COL = 4


def with_spikes(values, key, source, target, parts, factor):
    owner, partner = [(jnp.arange(values.shape[dim]) // (values.shape[dim] // parts)).reshape([-1 if axis == dim else 1 for axis in range(values.ndim)]) for dim in (source, target)]
    chosen = jax.random.permutation(key, parts)[partner]
    strong = (owner == chosen) | (owner == (partner + parts // 2) % parts)
    return jnp.where(strong, factor * values, values)


def level_of(own_key, shape, cuts, least, high):
    level, own = 1.0, jax.random.fold_in(own_key, 6)
    for axis_at, parts in cuts:
        heights = jnp.exp(jax.random.uniform(jax.random.fold_in(own, axis_at), (parts,), jnp.float32, least / len(cuts), high / len(cuts)))
        level = level * jnp.repeat(heights, shape[axis_at] // parts).reshape([-1 if axis == axis_at else 1 for axis in range(len(shape))])
    return level


def normal_values(own_key, shape, width, reach, split=(), held_as=jnp.bfloat16):
    values = width * jax.random.normal(own_key, shape, jnp.float32)
    if split:
        values = values * level_of(own_key, shape, split, -0.22, 0.18)
    return jnp.clip(values, -reach, reach).astype(held_as)


def gaussian_with(key, shape, deviation, limit, shards, heavy, kind=jnp.bfloat16):
    drawn = deviation * jax.random.normal(key, shape, jnp.float32)
    if shards:
        drawn = drawn * level_of(key, shape, shards, -0.22, 0.18)
    return jnp.clip(with_spikes(drawn, jax.random.fold_in(key, 3), *heavy), -limit, limit).astype(kind)


def setup_inputs(seed: int = 0) -> dict:
    keys = jax.random.split(jax.random.key(seed), 4)
    return {
        "points": normal_values(keys[0], (NPTS, FEAT), 1.0, 6.0, ((0, 32),)),
        "abar": gaussian_with(keys[1], (NPTS, N_ROW, N_COL, PTS), 1.0, 6.0, ((0, 8), (2, 4)), (2, 0, 4, 2.0)),
        "inv_scale": jnp.clip(jnp.exp(jax.random.uniform(keys[2], (FEAT,), jnp.float32, math.log(0.05), math.log(0.2))), 0.05, 0.2),
    }


def reference(points, abar, inv_scale):
    scaled = (points.astype(jnp.float32) * inv_scale[None, :]).astype(jnp.bfloat16)
    wide = scaled.astype(jnp.float32)
    squares = jnp.sum(wide * wide, axis=1)
    matrix = abar.reshape(NPTS, NPTS)
    block = 512 if NPTS % 512 == 0 else NPTS
    count = NPTS // block

    def one_block(carry, index):
        col_acc, col_total = carry
        start = (index * block).astype(jnp.int32)
        rows_scaled = lax.dynamic_slice_in_dim(scaled, start, block, 0)
        rows_sq = lax.dynamic_slice_in_dim(squares, start, block, 0)
        rows_ab = lax.dynamic_slice_in_dim(matrix, start, block, 0)
        inner = lax.dot_general(rows_scaled, scaled, (((1,), (1,)), ((), ())), preferred_element_type=jnp.float32)
        dist = rows_sq[:, None] + squares[None, :] - 2.0 * inner
        weighted = (rows_ab.astype(jnp.float32) * jnp.exp(-0.5 * dist)).astype(jnp.bfloat16)
        row_total = jnp.sum(weighted, axis=1, dtype=jnp.float32)
        first = row_total[:, None] * rows_scaled.astype(jnp.float32) - jnp.dot(weighted, scaled, preferred_element_type=jnp.float32)
        col_acc = col_acc + lax.dot_general(weighted, rows_scaled, (((0,), (0,)), ((), ())), preferred_element_type=jnp.float32)
        col_total = col_total + jnp.sum(weighted, axis=0, dtype=jnp.float32)
        return (col_acc, col_total), first

    init = (jnp.zeros((NPTS, FEAT), jnp.float32), jnp.zeros((NPTS,), jnp.float32))
    (col_acc, col_total), firsts = lax.scan(one_block, init, jnp.arange(count, dtype=jnp.int32))
    first = firsts.reshape(NPTS, FEAT)
    second = col_total[:, None] * wide - col_acc
    return -(first + second) * inv_scale[None, :]
```

```python
import jax
import jax.numpy as jnp
from jax import lax
from jax.experimental import pallas as pl
from jax.experimental.pallas import tpu as pltpu
from jax.sharding import PartitionSpec as P

F32, BF16 = jnp.float32, jnp.bfloat16
AXES = ("row", "col")
VMEM = pl.BlockSpec(memory_space=pltpu.VMEM)


def dest(i, k, n):
    return i ^ k if n & (n - 1) == 0 else (i + k) % n


def origin(i, k, n):
    return i ^ k if n & (n - 1) == 0 else (i + n - k) % n


def dot(a, b, over):
    return lax.dot_general(a, b, (over, ((), ())), preferred_element_type=F32)


def scaled_with_exponent(raw, inv, first):
    s = (raw.astype(F32) * inv).astype(BF16)
    wide = s.astype(F32)
    rest = -0.5 * jnp.sum(wide * wide, axis=1, keepdims=True)
    lane = lax.broadcasted_iota(jnp.int32, s.shape, 1)
    tail = jnp.zeros(s.shape, F32)
    for n in range(3):
        piece = rest.astype(BF16).astype(F32)
        rest = rest - piece
        tail = jnp.where(lane == (n if first else n + 3), piece, tail)
        tail = jnp.where(lane == (n + 3 if first else n), 1.0, tail)
    return s, tail.astype(BF16)


def local_kernel(lines, planes, steps, *refs):
    chip_ref, inv_ref, a_own, a_other = refs[:4]
    near = refs[4 : 4 + steps]
    far = refs[4 + steps]
    outs = refs[5 + steps : 6 + 2 * steps]
    left, right = refs[6 + 2 * steps :]
    core = lax.rem(lax.axis_index("row"), 2)
    plane = lax.div(lax.axis_index("row"), 2)
    line = lax.axis_index("col")
    width = chip_ref.shape[1]
    chip = chip_ref.shape[0]
    pts = chip // 2
    half = lines * pts
    inv = inv_ref[...]

    def put_left(at, raw):
        for c in range(2):
            s, tail = scaled_with_exponent(raw[c * pts : (c + 1) * pts], inv, True)
            rows = pl.ds(pl.multiple_of(c * half + at * pts, pts), pts)
            left[rows, :width] = s
            left[rows, width:] = tail

    def put_right(at, raw):
        s, tail = scaled_with_exponent(raw, inv, False)
        rows = pl.ds(pl.multiple_of(at * chip, chip), chip)
        right[rows, :width] = s
        right[rows, width:] = tail

    put_left(line, chip_ref[...])
    put_right(plane, chip_ref[...])

    def place(own_put, own_at, own_n, other_put, other_at, other_n):
        for k in range(1, steps + 1):
            if k < own_n:
                own_put(origin(own_at, k, own_n), near[k - 1][...])
            if k < other_n:
                other_put(origin(other_at, k, other_n), far[(k - 1) * chip : k * chip])

    ones = jnp.ones((chip, width), BF16)

    @pl.when(core == 1)
    def _():
        place(put_left, line, lines, put_right, plane, planes)
        for k in range(lines):
            at = dest(line, k, lines)
            for c in range(2):
                a_ref = a_own if c else a_other
                rows = pl.ds(pl.multiple_of(c * half + at * pts, pts), pts)
                lhs = left[rows, :]
                a_rows = pl.ds(pl.multiple_of(at * pts, pts), pts)
                total = jnp.zeros((pts, 2 * width), F32)
                for q in range(planes):
                    cols = slice(q * chip, (q + 1) * chip)
                    rhs = right[cols, :]
                    w = a_ref[a_rows, cols].astype(F32) * jnp.exp(dot(lhs, rhs, ((1,), (1,))))
                    total += dot(w.astype(BF16), jnp.concatenate([rhs[:, :width], ones], 1), ((1,), (0,)))
                value = total[:, width:] * lhs[:, :width].astype(F32) - total[:, :width]
                outs[k][c * pts : (c + 1) * pts, :] = value.astype(outs[k].dtype)
        for k in range(lines, steps + 1):
            outs[k][...] = jnp.zeros(outs[k].shape, outs[k].dtype)

    @pl.when(core == 0)
    def _():
        place(put_right, plane, planes, put_left, line, lines)
        for k in range(planes):
            at = dest(plane, k, planes)
            cols = pl.ds(pl.multiple_of(at * chip, chip), chip)
            rhs = right[cols, :]
            total = jnp.zeros((chip, 2 * width), F32)
            for c in range(2):
                a_ref = a_other if c else a_own
                for z in range(lines // 2):
                    rows = slice(c * half + z * chip, c * half + (z + 1) * chip)
                    lhs = left[rows, :]
                    a = a_ref[z * chip : (z + 1) * chip, cols].astype(F32)
                    w = a * jnp.exp(dot(lhs, rhs, ((1,), (1,))))
                    total += dot(w.astype(BF16), jnp.concatenate([lhs[:, :width], ones], 1), ((0,), (0,)))
            value = total[:, width:] * rhs[:, :width].astype(F32) - total[:, :width]
            outs[k][...] = value.astype(outs[k].dtype)
        for k in range(planes, steps + 1):
            outs[k][...] = jnp.zeros(outs[k].shape, outs[k].dtype)


def sum_kernel(*refs):
    terms, (keep, send) = refs[:-2], refs[-2:]
    core = lax.rem(lax.axis_index("row"), 2)
    pts = keep.shape[0]
    mine = pl.ds(pl.multiple_of(core * pts, pts), pts)
    other = pl.ds(pl.multiple_of((1 - core) * pts, pts), pts)
    for ref, rows in ((keep, mine), (send, other)):
        total = terms[0][rows, :].astype(F32)
        for term in terms[1:]:
            total += term[rows, :].astype(F32)
        ref[...] = total


def solution(mesh):
    rows, lines = mesh.shape["row"], mesh.shape["col"]
    planes = rows // 2
    steps = max(lines, planes) - 1

    def permute(value, target):
        pairs = []
        for r in range(rows):
            for c in range(lines):
                tr, tc = target(r, c)
                pairs.append((r * lines + c, tr * lines + tc))
        return lax.ppermute(value, AXES, pairs)

    def swap(value):
        return permute(value, lambda r, c: (r ^ 1, c))

    def exchange(value, k):
        along_col = (k - 1) % (lines - 1) + 1
        along_row = (k - 1) % (planes - 1) + 1

        def target(r, c):
            if r % 2:
                return r, dest(c, along_col, lines)
            return 2 * dest(r // 2, along_row, planes), c

        return permute(value, target)

    def per_device(points, abar, inv_scale):
        pts, width = points.shape
        core = lax.axis_index("row") % 2
        inv = inv_scale[None, :]
        other = swap(points)
        chip = jnp.where(
            core == 0, jnp.concatenate([points, other], 0), jnp.concatenate([other, points], 0)
        )
        tile = abar.reshape(abar.shape[0], -1)
        near = [exchange(chip, k) for k in range(steps, 0, -1)][::-1]
        tile_other = swap(tile)
        far = swap(jnp.concatenate(near, 0))
        outs = pl.pallas_call(
            lambda *refs: local_kernel(lines, planes, steps, *refs),
            out_shape=[jax.ShapeDtypeStruct((2 * pts, width), BF16)] * (steps + 1),
            in_specs=[VMEM] * (5 + steps),
            out_specs=[VMEM] * (steps + 1),
            scratch_shapes=[
                pltpu.VMEM((lines * 2 * pts, 2 * width), BF16),
                pltpu.VMEM((planes * 2 * pts, 2 * width), BF16),
            ],
            name="local",
        )(chip, inv, tile, tile_other, *near, far)
        got = [exchange(outs[k], k) for k in range(steps, 0, -1)]
        keep, send = pl.pallas_call(
            sum_kernel,
            out_shape=[jax.ShapeDtypeStruct((pts, width), F32)] * 2,
            in_specs=[VMEM] * (steps + 1),
            out_specs=[VMEM] * 2,
            name="total",
        )(outs[0], *got)
        return -(keep + swap(send)) * inv

    placed = (P(("row", "col"), None), P("row", None, "col", None), P())
    return jax.shard_map(
        per_device, mesh=mesh, in_specs=placed, out_specs=P(("row", "col"), None), check_vma=False
    )
```

```python
import jax
import jax.numpy as jnp
from jax import lax
from jax.experimental import pallas as pl
from jax.experimental.pallas import tpu as pltpu
from jax.sharding import PartitionSpec as P


F32, BF16 = jnp.float32, jnp.bfloat16
AXES = ("row", "col")
VMEM = pl.BlockSpec(memory_space=pltpu.VMEM)


def dest(i, k, n):
    return i ^ k if n & (n - 1) == 0 else (i + k) % n


def origin(i, k, n):
    return i ^ k if n & (n - 1) == 0 else (i + n - k) % n


def dot(a, b, over):
    return lax.dot_general(a, b, (over, ((), ())), preferred_element_type=F32)


def scaled_with_exponent(raw, inv, first):
    s = (raw.astype(F32) * inv).astype(BF16)
    wide = s.astype(F32)
    rest = -0.5 * jnp.sum(wide * wide, axis=1, keepdims=True)
    lane = lax.broadcasted_iota(jnp.int32, s.shape, 1)
    tail = jnp.zeros(s.shape, F32)
    for n in range(3):
        piece = rest.astype(BF16).astype(F32)
        rest = rest - piece
        tail = jnp.where(lane == (n if first else n + 3), piece, tail)
        tail = jnp.where(lane == (n + 3 if first else n), 1.0, tail)
    return s, tail.astype(BF16)


def local_kernel(lines, planes, steps, *refs):
    chip_ref, inv_ref, a_own, a_other = refs[:4]
    near = refs[4 : 4 + steps]
    far = refs[4 + steps]
    outs = refs[5 + steps : 6 + 2 * steps]
    left, right = refs[6 + 2 * steps :]
    core = lax.rem(lax.axis_index("row"), 2)
    plane = lax.div(lax.axis_index("row"), 2)
    line = lax.axis_index("col")
    width = chip_ref.shape[1]
    chip = chip_ref.shape[0]
    pts = chip // 2
    half = lines * pts
    inv = inv_ref[...]

    def put_left(at, raw):
        for c in range(2):
            s, tail = scaled_with_exponent(raw[c * pts : (c + 1) * pts], inv, True)
            rows = pl.ds(pl.multiple_of(c * half + at * pts, pts), pts)
            left[rows, :width] = s
            left[rows, width:] = tail

    def put_right(at, raw):
        s, tail = scaled_with_exponent(raw, inv, False)
        rows = pl.ds(pl.multiple_of(at * chip, chip), chip)
        right[rows, :width] = s
        right[rows, width:] = tail

    put_left(line, chip_ref[...])
    put_right(plane, chip_ref[...])

    def place(own_put, own_at, own_n, other_put, other_at, other_n):
        for k in range(1, steps + 1):
            if k < own_n:
                own_put(origin(own_at, k, own_n), near[k - 1][...])
            if k < other_n:
                other_put(origin(other_at, k, other_n), far[(k - 1) * chip : k * chip])

    ones = jnp.ones((chip, width), BF16)

    @pl.when(core == 1)
    def _():
        place(put_left, line, lines, put_right, plane, planes)
        for k in range(lines):
            at = dest(line, k, lines)
            for c in range(2):
                a_ref = a_own if c else a_other
                rows = pl.ds(pl.multiple_of(c * half + at * pts, pts), pts)
                lhs = left[rows, :]
                a_rows = pl.ds(pl.multiple_of(at * pts, pts), pts)
                total = jnp.zeros((pts, 2 * width), F32)
                for q in range(planes):
                    cols = slice(q * chip, (q + 1) * chip)
                    rhs = right[cols, :]
                    w = a_ref[a_rows, cols].astype(F32) * jnp.exp(dot(lhs, rhs, ((1,), (1,))))
                    total += dot(w.astype(BF16), jnp.concatenate([rhs[:, :width], ones], 1), ((1,), (0,)))
                value = total[:, width:] * lhs[:, :width].astype(F32) - total[:, :width]
                outs[k][c * pts : (c + 1) * pts, :] = value.astype(outs[k].dtype)
        for k in range(lines, steps + 1):
            outs[k][...] = jnp.zeros(outs[k].shape, outs[k].dtype)

    @pl.when(core == 0)
    def _():
        place(put_right, plane, planes, put_left, line, lines)
        for k in range(planes):
            at = dest(plane, k, planes)
            cols = pl.ds(pl.multiple_of(at * chip, chip), chip)
            rhs = right[cols, :]
            total = jnp.zeros((chip, 2 * width), F32)
            for c in range(2):
                a_ref = a_other if c else a_own
                for z in range(lines // 2):
                    rows = slice(c * half + z * chip, c * half + (z + 1) * chip)
                    lhs = left[rows, :]
                    a = a_ref[z * chip : (z + 1) * chip, cols].astype(F32)
                    w = a * jnp.exp(dot(lhs, rhs, ((1,), (1,))))
                    total += dot(w.astype(BF16), jnp.concatenate([lhs[:, :width], ones], 1), ((0,), (0,)))
            value = total[:, width:] * rhs[:, :width].astype(F32) - total[:, :width]
            outs[k][...] = value.astype(outs[k].dtype)
        for k in range(planes, steps + 1):
            outs[k][...] = jnp.zeros(outs[k].shape, outs[k].dtype)


def sum_kernel(*refs):
    terms, (keep, send) = refs[:-2], refs[-2:]
    core = lax.rem(lax.axis_index("row"), 2)
    pts = keep.shape[0]
    mine = pl.ds(pl.multiple_of(core * pts, pts), pts)
    other = pl.ds(pl.multiple_of((1 - core) * pts, pts), pts)
    for ref, rows in ((keep, mine), (send, other)):
        total = terms[0][rows, :].astype(F32)
        for term in terms[1:]:
            total += term[rows, :].astype(F32)
        ref[...] = total


def solution(mesh):
    rows, lines = mesh.shape["row"], mesh.shape["col"]
    planes = rows // 2
    steps = max(lines, planes) - 1

    def permute(value, target):
        pairs = []
        for r in range(rows):
            for c in range(lines):
                tr, tc = target(r, c)
                pairs.append((r * lines + c, tr * lines + tc))
        return lax.ppermute(value, AXES, pairs)

    def swap(value):
        return permute(value, lambda r, c: (r ^ 1, c))

    def exchange(value, k):
        along_col = (k - 1) % (lines - 1) + 1
        along_row = (k - 1) % (planes - 1) + 1

        def target(r, c):
            if r % 2:
                return r, dest(c, along_col, lines)
            return 2 * dest(r // 2, along_row, planes), c

        return permute(value, target)

    def local_part(points, abar, inv_scale):
        pts, width = points.shape
        core = lax.axis_index("row") % 2
        inv = inv_scale[None, :]
        grant = 8 * 2**20 + 2 * pts * width * 2 * (lines + planes) * 2
        other = swap(points)
        chip = lax.dynamic_update_slice(
            jnp.zeros((2 * pts, width), points.dtype), points, (core * pts, 0)
        )
        chip = lax.dynamic_update_slice(chip, other, ((1 - core) * pts, 0))
        near = []
        for k in range(steps, 0, -1):
            near.insert(0, exchange(chip, k))
        abar, _ = lax.optimization_barrier((abar, chip))
        tile = abar.reshape(abar.shape[0], -1)
        tile_other = swap(tile)
        far = swap(jnp.concatenate(near, 0))
        outs = pl.pallas_call(
            lambda *refs: local_kernel(lines, planes, steps, *refs),
            out_shape=[jax.ShapeDtypeStruct((2 * pts, width), BF16)] * (steps + 1),
            in_specs=[VMEM] * (5 + steps),
            out_specs=[VMEM] * (steps + 1),
            scratch_shapes=[
                pltpu.VMEM((lines * 2 * pts, 2 * width), BF16),
                pltpu.VMEM((planes * 2 * pts, 2 * width), BF16),
            ],
            compiler_params=pltpu.CompilerParams(vmem_limit_bytes=grant),
            name="local",
        )(chip, inv, tile, tile_other, *near, far)
        got = [exchange(outs[k], k) for k in range(steps, 0, -1)]
        keep, send = pl.pallas_call(
            sum_kernel,
            out_shape=[jax.ShapeDtypeStruct((pts, width), F32)] * 2,
            in_specs=[VMEM] * (steps + 1),
            out_specs=[VMEM] * 2,
            compiler_params=pltpu.CompilerParams(vmem_limit_bytes=grant // 2),
            name="total",
        )(outs[0], *got)
        return -(keep + swap(send)) * inv

    placed = (P(("row", "col"), None), P("row", None, "col", None), P())
    return jax.shard_map(
        local_part, mesh=mesh, in_specs=placed, out_specs=P(("row", "col"), None), check_vma=False
    )
```

```python
import jax
import jax.numpy as jnp
from jax import lax
from jax.experimental import pallas as pl
from jax.experimental.pallas import tpu as pltpu
from jax.sharding import PartitionSpec as P


F32, BF16 = jnp.float32, jnp.bfloat16
AXES = ("row", "col")
VMEM = pl.BlockSpec(memory_space=pltpu.VMEM)
OVER_LAST, OVER_FIRST, PLAIN = ((1,), (1,)), ((0,), (0,)), ((1,), (0,))


def partner(i, distance, n):
    return i ^ distance if n & (n - 1) == 0 else (i + distance) % n


def origin(i, distance, n):
    return i ^ distance if n & (n - 1) == 0 else lax.rem(i + n - distance, n)


def dot(a, b, over):
    return lax.dot_general(a, b, (over, ((), ())), preferred_element_type=F32)


def augmented(raw, inv, first):
    s = (raw.astype(F32) * inv).astype(BF16)
    wide = s.astype(F32)
    rest = -0.5 * jnp.sum(wide * wide, axis=1, keepdims=True)
    lane = lax.broadcasted_iota(jnp.int32, s.shape, 1)
    tail = jnp.zeros(s.shape, F32)
    for n in range(3):
        piece = rest.astype(BF16).astype(F32)
        rest = rest - piece
        tail = jnp.where(lane == (n if first else n + 3), piece, tail)
        tail = jnp.where(lane == (n + 3 if first else n), 1.0, tail)
    return jnp.concatenate([s, tail.astype(BF16)], 1)


class Layout:
    def __init__(self, lines, planes, pts, width):
        self.lines, self.planes, self.pts, self.width = lines, planes, pts, width
        self.steps = max(lines, planes) - 1
        self.chip = 2 * pts

    def distance(self, k):
        return self.steps + 1 - k

    def valid(self, k, n):
        return k == 0 or self.distance(k) < n

    def here(self):
        row = lax.axis_index("row")
        return lax.axis_index("col"), lax.div(row, 2), lax.rem(row, 2)

    def rows(self, k):
        return slice(k * self.chip, (k + 1) * self.chip)

    def weights(self, tiles, line, plane, exponent):
        at = pl.ds(pl.multiple_of(line * self.pts, self.pts), self.pts)
        cols = pl.ds(pl.multiple_of(plane * self.chip, self.chip), self.chip)
        a = jnp.concatenate([tile[at, cols] for tile in tiles], 0)
        return (a.astype(F32) * jnp.exp(exponent)).astype(BF16)

    def term(self, core, tiles, mine, mine_at, theirs, theirs_at):
        side = jnp.concatenate([theirs[:, : self.width], jnp.ones((self.chip, self.width), BF16)], 1)
        if core:
            w = self.weights(tiles, mine_at, theirs_at, dot(mine, theirs, OVER_LAST))
            return dot(w, side, PLAIN)
        w = self.weights(tiles, theirs_at, mine_at, dot(theirs, mine, OVER_LAST))
        return dot(w, side, OVER_FIRST)

    def on_each_core(self, body):
        line, plane, core = self.here()
        for c in (0, 1):
            own, other = ((plane, self.planes), (line, self.lines))[:: 1 if c == 0 else -1]

            @pl.when(core == c)
            def _(c=c, own=own, other=other):
                body(c, *own, *other)

    def early(self, chip, inv, near, a_own, a_other, mine, part):
        def body(core, own, own_n, other, other_n):
            tiles = (a_other, a_own) if core else (a_own, a_other)
            theirs = augmented(chip[...], inv[...], not core)
            for k in range(self.steps + 1):
                if not self.valid(k, own_n):
                    continue
                raw = near[self.rows(k - 1), :] if k else chip[...]
                block = augmented(raw, inv[...], bool(core))
                mine[self.rows(k), :] = block
                at = origin(own, self.distance(k), own_n) if k else own
                part[self.rows(k), :] = self.term(core, tiles, block, at, theirs, other)

        self.on_each_core(body)

    def finished(self, k, core, tiles, theirs, mine, part, own, own_n, other, other_n):
        block = mine[self.rows(k), :]
        at = origin(own, self.distance(k), own_n) if k else own
        total = part[self.rows(k), :]
        for j in range(1, self.steps + 1):
            if self.valid(j, other_n):
                from_at = origin(other, self.distance(j), other_n)
                total += self.term(core, tiles, block, at, theirs[self.rows(j - 1), :], from_at)
        return total[:, self.width :] * block[:, : self.width].astype(F32) - total[:, : self.width]

    def send(self, far, inv, mine, part, a_own, a_other, theirs, *outs):
        def body(core, own, own_n, other, other_n):
            tiles = (a_other, a_own) if core else (a_own, a_other)
            for j in range(1, self.steps + 1):
                if self.valid(j, other_n):
                    theirs[self.rows(j - 1), :] = augmented(far[self.rows(j - 1), :], inv[...], not core)
            for k in range(1, self.steps + 1):
                out = outs[k - 1]
                if self.valid(k, own_n):
                    value = self.finished(k, core, tiles, theirs, mine, part, own, own_n, other, other_n)
                    out[...] = value.astype(out.dtype)
                else:
                    out[...] = jnp.zeros(out.shape, out.dtype)

        self.on_each_core(body)

    def keep(self, theirs, mine, part, a_own, a_other, out):
        def body(core, own, own_n, other, other_n):
            tiles = (a_other, a_own) if core else (a_own, a_other)
            out[...] = self.finished(0, core, tiles, theirs, mine, part, own, own_n, other, other_n)

        self.on_each_core(body)

    def total(self, *refs):
        terms, (keep, send) = refs[:-2], refs[-2:]
        core = self.here()[2]
        mine = pl.ds(pl.multiple_of(core * self.pts, self.pts), self.pts)
        other = pl.ds(pl.multiple_of((1 - core) * self.pts, self.pts), self.pts)
        for ref, rows in ((keep, mine), (send, other)):
            acc = terms[0][rows, :].astype(F32)
            for term in terms[1:]:
                acc += term[rows, :].astype(F32)
            ref[...] = acc


def solution(mesh):
    rows, lines = mesh.shape["row"], mesh.shape["col"]
    planes = rows // 2
    steps = max(lines, planes) - 1

    def permute(value, target):
        pairs = []
        for r in range(rows):
            for c in range(lines):
                tr, tc = target(r, c)
                pairs.append((r * lines + c, tr * lines + tc))
        return lax.ppermute(value, AXES, pairs)

    def swap(value):
        return permute(value, lambda r, c: (r ^ 1, c))

    def exchange(value, k):
        distance = steps + 1 - k

        def target(r, c):
            if r % 2:
                return r, partner(c, (distance - 1) % (lines - 1) + 1, lines)
            return 2 * partner(r // 2, (distance - 1) % (planes - 1) + 1, planes), c

        return permute(value, target)

    def local_part(points, abar, inv_scale):
        pts, width = points.shape
        lay = Layout(lines, planes, pts, width)
        chip_rows = lay.chip
        core = lax.axis_index("row") % 2
        inv = inv_scale[None, :]
        grant = pltpu.CompilerParams(vmem_limit_bytes=(6 + steps) * 2**20)

        def call(body, outs, *args):
            return pl.pallas_call(
                body,
                out_shape=[jax.ShapeDtypeStruct(s, t) for s, t in outs],
                in_specs=[VMEM] * len(args),
                out_specs=[VMEM] * len(outs),
                compiler_params=grant,
            )(*args)

        other = swap(points)
        abar_other = swap(abar)
        chip = lax.dynamic_update_slice(
            jnp.zeros((chip_rows, width), points.dtype), points, (core * pts, 0)
        )
        chip = lax.dynamic_update_slice(chip, other, ((1 - core) * pts, 0))
        near = []
        for k in range(1, steps + 1):
            near.append(exchange(chip, k))
        abar, _ = lax.optimization_barrier((abar, chip))
        tiles = [a.reshape(a.shape[0], -1).astype(F32) for a in (abar, abar_other)]
        near = jnp.concatenate(near, 0)
        far = swap(near)
        blocks = (steps + 1) * chip_rows
        mine, part = call(lay.early, [((blocks, 2 * width), BF16), ((blocks, 2 * width), F32)], chip, inv, near, *tiles)
        theirs, *outs = call(
            lay.send,
            [((steps * chip_rows, 2 * width), BF16)] + [((chip_rows, width), BF16)] * steps,
            far,
            inv,
            mine,
            part,
            *tiles,
        )
        got = []
        for k in range(1, steps + 1):
            got.append(exchange(outs[k - 1], k))
        (out,) = call(lay.keep, [((chip_rows, width), F32)], theirs, mine, part, *tiles)
        keep, send = call(lay.total, [((pts, width), F32)] * 2, out, *got)
        return -(keep + swap(send)) * inv

    placed = (P(("row", "col"), None), P("row", None, "col", None), P())
    return jax.shard_map(local_part, mesh=mesh, in_specs=placed, out_specs=P(("row", "col"), None), check_vma=False)
```

```python
import jax
import jax.numpy as jnp
from jax import lax
from jax.experimental import pallas as pl
from jax.experimental.pallas import tpu as pltpu
from jax.sharding import PartitionSpec as P


F32, BF16 = jnp.float32, jnp.bfloat16
AXES = ("row", "col")
VMEM = pl.BlockSpec(memory_space=pltpu.VMEM)
OVER_LAST, OVER_FIRST, PLAIN = ((1,), (1,)), ((0,), (0,)), ((1,), (0,))


def partner(i, distance, n):
    return i ^ distance if n & (n - 1) == 0 else (i + distance) % n


def origin(i, distance, n):
    return i ^ distance if n & (n - 1) == 0 else lax.rem(i + n - distance, n)


def dot(a, b, over):
    return lax.dot_general(a, b, (over, ((), ())), preferred_element_type=F32)


def augmented(raw, inv, first):
    s = (raw.astype(F32) * inv).astype(BF16)
    wide = s.astype(F32)
    rest = -0.5 * jnp.sum(wide * wide, axis=1, keepdims=True)
    lane = lax.broadcasted_iota(jnp.int32, s.shape, 1)
    tail = jnp.zeros(s.shape, F32)
    for n in range(3):
        piece = rest.astype(BF16).astype(F32)
        rest = rest - piece
        tail = jnp.where(lane == (n if first else n + 3), piece, tail)
        tail = jnp.where(lane == (n + 3 if first else n), 1.0, tail)
    return jnp.concatenate([s, tail.astype(BF16)], 1)


def relayout(wide, deep, own, other, own_out, other_out, spare):
    width = own.shape[1]
    at = 0
    for ref, out in ((own, own_out), (other, other_out)):
        for start in range(0, out.shape[0], deep):
            spare[at] = ref[start * wide : (start + deep) * wide, :].astype(F32)
            for a in range(wide):
                rows = spare[at, pl.ds(a, deep, stride=wide), :]
                out[start : start + deep, a * width : (a + 1) * width] = rows
            at = 1 - at


class Layout:
    def __init__(self, lines, planes, pts, width):
        self.lines, self.planes, self.pts, self.width = lines, planes, pts, width
        self.steps = max(lines, planes) - 1
        self.chip = 2 * pts

    def here(self):
        row = lax.axis_index("row")
        return lax.axis_index("col"), lax.div(row, 2), lax.rem(row, 2)

    def rows(self, k, n=1):
        return pl.ds(k * self.chip, n * self.chip)

    def blocks(self, side, lo, hi):
        n = (self.planes, self.lines)[side]
        return [k for k in range(lo, hi) if k == 0 or self.steps + 1 - k < n]

    def groups(self, side, lo, hi):
        have = self.blocks(side, lo, hi)
        return [have[i : i + 3] for i in range(0, len(have), 3)]

    def piece(self, tiles, line, plane):
        at = pl.ds(pl.multiple_of(line * self.pts, self.pts), self.pts)
        cols = pl.ds(pl.multiple_of(plane * self.chip, self.chip), self.chip)
        return jnp.concatenate([tile[at, cols] for tile in tiles], 0)

    def term(self, core, tiles, mine, at, theirs, theirs_at):
        side = jnp.concatenate([theirs[:, : self.width], jnp.ones((self.chip, self.width), BF16)], 1)
        if core:
            e = jnp.exp(dot(mine, theirs, OVER_LAST))
            a = jnp.concatenate([self.piece(tiles, k, theirs_at) for k in at], 0)
            w = (a * e).astype(BF16)
            return dot(w, side, PLAIN)
        e = jnp.exp(dot(theirs, mine, OVER_LAST))
        a = jnp.concatenate([self.piece(tiles, theirs_at, k) for k in at], 1)
        w = (a * e).astype(BF16)
        return dot(w, side, OVER_FIRST)

    def on_each_core(self, body):
        line, plane, core = self.here()
        for c in (0, 1):

            def chip_of(side, k, line=line, plane=plane):
                here, n = ((plane, self.planes), (line, self.lines))[side]
                return origin(here, self.steps + 1 - k, n) if k else here

            @pl.when(core == c)
            def _(c=c, chip_of=chip_of):
                body(c, chip_of)

    def add(self, core, chip_of, tiles, mine, ks, theirs, j):
        return self.term(
            core, tiles, mine, [chip_of(core, k) for k in ks], theirs, chip_of(1 - core, j)
        )

    def early(self, chip, inv, near, a_own, a_other, mine, theirs, part):
        def body(core, chip_of):
            tiles = (a_other, a_own) if core else (a_own, a_other)
            side = augmented(chip[...], inv[...], not core)
            theirs[...] = side
            for k in self.blocks(core, 0, 2):
                block = augmented(near[...] if k else chip[...], inv[...], bool(core))
                mine[self.rows(k), :] = block
                part[self.rows(k), :] = self.add(core, chip_of, tiles, block, [k], side, 0)

        self.on_each_core(body)

    def middle(self, inv, near, far, mine0, theirs0, part0, a_own, a_other, mine, first, part):
        def body(core, chip_of):
            tiles = (a_other, a_own) if core else (a_own, a_other)
            sides = [(0, theirs0[...])]
            for j in self.blocks(1 - core, 1, 2):
                sides.append((j, augmented(far[...], inv[...], not core)))
            for ks in self.groups(core, 2, self.steps + 1):
                rows = self.rows(ks[0] - 2, len(ks))
                block = augmented(near[rows, :], inv[...], bool(core))
                mine[rows, :] = block
                total = self.add(core, chip_of, tiles, block, ks, sides[0][1], 0)
                for j, side in sides[1:]:
                    total += self.add(core, chip_of, tiles, block, ks, side, j)
                part[rows, :] = total
            ks = self.blocks(core, 0, 2)
            rows = self.rows(0, len(ks))
            total = part0[rows, :]
            for j, side in sides[1:]:
                total += self.add(core, chip_of, tiles, mine0[rows, :], ks, side, j)
            first[rows, :] = total

        self.on_each_core(body)

    def closed(self, block, total):
        return total[:, self.width :] * block[:, : self.width].astype(F32) - total[:, : self.width]

    def send(self, inv, far, mine0, mine, first, part, a_own, a_other, theirs, *outs):
        def body(core, chip_of):
            tiles = (a_other, a_own) if core else (a_own, a_other)
            have = self.blocks(1 - core, 2, self.steps + 1)
            few = len(have) <= 3
            sides = {}
            for j in have:
                sides[j] = augmented(far[self.rows(j - 2), :], inv[...], not core)
                theirs[self.rows(j - 2), :] = sides[j]
            for k in range(1, self.steps + 1):
                if k not in self.blocks(core, 1, self.steps + 1):
                    outs[k - 1][...] = jnp.zeros(outs[k - 1].shape, outs[k - 1].dtype)
            for ks in self.groups(core, 1, self.steps + 1):
                parts = [(mine0, first, k) if k == 1 else (mine, part, k - 2) for k in ks]
                block = jnp.concatenate([m[self.rows(at), :] for m, _, at in parts], 0)
                total = jnp.concatenate([p[self.rows(at), :] for _, p, at in parts], 0)
                if few:
                    for j in have:
                        total += self.add(core, chip_of, tiles, block, ks, sides[j], j)
                else:
                    total = self.rest(core, chip_of, tiles, block, ks, theirs, have, total)
                value = self.closed(block, total)
                for n, k in enumerate(ks):
                    out = outs[k - 1]
                    out[...] = value[n * self.chip : (n + 1) * self.chip].astype(out.dtype)

        self.on_each_core(body)

    def rest(self, core, chip_of, tiles, block, ks, theirs, have, total):
        def step(j, total):
            rows = pl.ds(pl.multiple_of((j - 2) * self.chip, self.chip), self.chip)
            side = theirs[rows, :]
            line, plane, _ = self.here()
            here, n = (plane, self.planes) if core else (line, self.lines)
            from_at = origin(here, self.steps + 1 - j, n)
            at = [chip_of(core, k) for k in ks]
            return total + self.term(core, tiles, block, at, side, from_at)

        return lax.fori_loop(have[0], have[-1] + 1, step, total)

    def keep(self, mine0, first, theirs, a_own, a_other, out):
        def body(core, chip_of):
            tiles = (a_other, a_own) if core else (a_own, a_other)
            block, total = mine0[self.rows(0), :], first[self.rows(0), :]
            have = self.blocks(1 - core, 2, self.steps + 1)
            if len(have) <= 3:
                for j in have:
                    total += self.add(core, chip_of, tiles, block, [0], theirs[self.rows(j - 2), :], j)
            else:
                total = self.rest(core, chip_of, tiles, block, [0], theirs, have, total)
            out[...] = self.closed(block, total)

        self.on_each_core(body)

    def total(self, *refs):
        terms, (keep, send) = refs[:-2], refs[-2:]
        core = self.here()[2]
        mine = pl.ds(pl.multiple_of(core * self.pts, self.pts), self.pts)
        other = pl.ds(pl.multiple_of((1 - core) * self.pts, self.pts), self.pts)
        for ref, rows in ((keep, mine), (send, other)):
            acc = terms[0][rows, :].astype(F32)
            for term in terms[1:]:
                acc += term[rows, :].astype(F32)
            ref[...] = acc


def solution(mesh):
    rows, lines = mesh.shape["row"], mesh.shape["col"]
    planes = rows // 2
    steps = max(lines, planes) - 1

    def permute(value, target):
        pairs = []
        for r in range(rows):
            for c in range(lines):
                tr, tc = target(r, c)
                pairs.append((r * lines + c, tr * lines + tc))
        return lax.ppermute(value, AXES, pairs)

    def swap(value):
        return permute(value, lambda r, c: (r ^ 1, c))

    def exchange(value, k):
        distance = steps + 1 - k

        def target(r, c):
            if r % 2:
                return r, partner(c, (distance - 1) % (lines - 1) + 1, lines)
            return 2 * partner(r // 2, (distance - 1) % (planes - 1) + 1, planes), c

        return permute(value, target)

    def local_part(points, abar, inv_scale):
        pts, width = points.shape
        lay = Layout(lines, planes, pts, width)
        chip_rows = lay.chip
        core = lax.axis_index("row") % 2
        inv = inv_scale[None, :]
        grant = pltpu.CompilerParams(vmem_limit_bytes=(6 + steps) * 2**20)

        def call(body, outs, *args):
            return pl.pallas_call(
                body,
                out_shape=[jax.ShapeDtypeStruct(s, t) for s, t in outs],
                in_specs=[VMEM] * len(args),
                out_specs=[VMEM] * len(outs),
                compiler_params=grant,
            )(*args)

        other = swap(points)
        abar_other = swap(abar)
        chip = lax.dynamic_update_slice(
            jnp.zeros((chip_rows, width), points.dtype), points, (core * pts, 0)
        )
        chip = lax.dynamic_update_slice(chip, other, ((1 - core) * pts, 0))
        near = []
        for k in range(1, steps + 1):
            near.append(exchange(chip, k))
        count, wide = abar.shape[0], abar.shape[1] * abar.shape[2]
        cells = [a.reshape(count * wide, abar.shape[3]) for a in (abar, abar_other)]
        if count <= 8 * pts:
            deep = 128
            tiles = pl.pallas_call(
                lambda *refs: relayout(wide, deep, *refs),
                out_shape=[jax.ShapeDtypeStruct((count, wide * width), F32)] * 2,
                in_specs=[VMEM] * 2,
                out_specs=[VMEM] * 2,
                scratch_shapes=[pltpu.VMEM((2, deep * wide, width), F32)],
                compiler_params=grant,
                name="relayout",
            )(*cells)
        else:
            tiles = [a.reshape(count, wide * width).astype(F32) for a in cells]
        far1 = swap(near[0])
        after = jnp.concatenate(near[1:], 0)
        far2 = swap(after)
        deep = 2 * width
        mine0, theirs0, part0 = call(
            lay.early,
            [((2 * chip_rows, deep), BF16), ((chip_rows, deep), BF16), ((2 * chip_rows, deep), F32)],
            chip,
            inv,
            near[0],
            *tiles,
        )
        rest_rows = (steps - 1) * chip_rows
        mine, first, part = call(
            lay.middle,
            [
                ((rest_rows, deep), BF16),
                ((2 * chip_rows, deep), F32),
                ((rest_rows, deep), F32),
            ],
            inv,
            after,
            far1,
            mine0,
            theirs0,
            part0,
            *tiles,
        )
        theirs, *outs = call(
            lay.send,
            [((rest_rows, deep), BF16)] + [((chip_rows, width), BF16)] * steps,
            inv,
            far2,
            mine0,
            mine,
            first,
            part,
            *tiles,
        )
        got = []
        for k in range(1, steps + 1):
            got.append(exchange(outs[k - 1], k))
        (out,) = call(lay.keep, [((chip_rows, width), F32)], mine0, first, theirs, *tiles)
        keep, send = call(lay.total, [((pts, width), F32)] * 2, out, *got)
        return -(keep + swap(send)) * inv

    placed = (P(("row", "col"), None), P("row", None, "col", None), P())
    return jax.shard_map(
        local_part, mesh=mesh, in_specs=placed, out_specs=P(("row", "col"), None), check_vma=False
    )
```

```python
import jax
import jax.numpy as jnp
from jax import lax
from jax.experimental import pallas as pl
from jax.experimental.pallas import tpu as pltpu
from jax.sharding import PartitionSpec as P


F32, BF16 = jnp.float32, jnp.bfloat16
AXES = ("row", "col")
VMEM = pl.BlockSpec(memory_space=pltpu.VMEM)
OVER_LAST, OVER_FIRST, PLAIN = ((1,), (1,)), ((0,), (0,)), ((1,), (0,))


def partner(i, distance, n):
    return i ^ distance if n & (n - 1) == 0 else (i + distance) % n


def origin(i, distance, n):
    return i ^ distance if n & (n - 1) == 0 else lax.rem(i + n - distance, n)


def dot(a, b, over):
    return lax.dot_general(a, b, (over, ((), ())), preferred_element_type=F32)


def augmented(raw, inv, first):
    s = (raw.astype(F32) * inv).astype(BF16)
    wide = s.astype(F32)
    rest = -0.5 * jnp.sum(wide * wide, axis=1, keepdims=True)
    lane = lax.broadcasted_iota(jnp.int32, s.shape, 1)
    at, ones = (0, 3) if first else (3, 0)
    tail = jnp.where((lane >= ones) & (lane < ones + 3), 1.0, 0.0)
    for n in range(3):
        tail = jnp.where(lane == at + n, rest, tail)
        rest = rest - rest.astype(BF16).astype(F32)
    return jnp.concatenate([s, tail.astype(BF16)], 1)


def relayout(wide, deep, own, other, own_out, other_out, spare):
    width = own.shape[1]
    at = 0
    for ref, out in ((own, own_out), (other, other_out)):
        for start in range(0, out.shape[0], deep):
            spare[at] = ref[start * wide : (start + deep) * wide, :].astype(F32)
            for a in range(wide):
                rows = spare[at, pl.ds(a, deep, stride=wide), :]
                out[start : start + deep, a * width : (a + 1) * width] = rows
            at = 1 - at


class Layout:
    def __init__(self, lines, planes, pts, width):
        self.lines, self.planes, self.pts, self.width = lines, planes, pts, width
        self.steps = max(lines, planes) - 1
        self.chip = 2 * pts

    def here(self):
        row = lax.axis_index("row")
        return lax.axis_index("col"), lax.div(row, 2), lax.rem(row, 2)

    def rows(self, k, n=1):
        return pl.ds(k * self.chip, n * self.chip)

    def blocks(self, side, lo, hi):
        n = (self.planes, self.lines)[side]
        return [k for k in range(lo, hi) if k == 0 or self.steps + 1 - k < n]

    def groups(self, side, lo, hi):
        have = self.blocks(side, lo, hi)
        return [have[i : i + 3] for i in range(0, len(have), 3)]

    def piece(self, tiles, line, plane):
        at = pl.ds(pl.multiple_of(line * self.pts, self.pts), self.pts)
        cols = pl.ds(pl.multiple_of(plane * self.chip, self.chip), self.chip)
        return jnp.concatenate([tile[at, cols] for tile in tiles], 0)

    def term(self, core, tiles, mine, at, theirs, theirs_at):
        if not core and len(at) > 1 and len(theirs_at) > 1:
            parts = []
            for n, j in enumerate(theirs_at):
                rows = theirs[n * self.chip : (n + 1) * self.chip]
                parts.append(self.term(core, tiles, mine, at, rows, [j]))
            return sum(parts[1:], parts[0])
        ones = jnp.ones((theirs.shape[0], self.width), BF16)
        side = jnp.concatenate([theirs[:, : self.width], ones], 1)
        if core:
            e = jnp.exp(dot(mine, theirs, OVER_LAST))
            rows = [[self.piece(tiles, k, j) for j in theirs_at] for k in at]
        else:
            e = jnp.exp(dot(theirs, mine, OVER_LAST))
            rows = [[self.piece(tiles, j, k) for k in at] for j in theirs_at]
        a = jnp.concatenate([jnp.concatenate(row, 1) for row in rows], 0)
        return dot((a * e).astype(BF16), side, PLAIN if core else OVER_FIRST)

    def on_each_core(self, body):
        line, plane, core = self.here()
        for c in (0, 1):

            def chip_of(side, k, line=line, plane=plane):
                here, n = ((plane, self.planes), (line, self.lines))[side]
                return origin(here, self.steps + 1 - k, n) if k else here

            @pl.when(core == c)
            def _(c=c, chip_of=chip_of):
                body(c, chip_of)

    def add(self, core, chip_of, tiles, mine, ks, theirs, js):
        at, from_at = [chip_of(core, k) for k in ks], [chip_of(1 - core, j) for j in js]
        return self.term(core, tiles, mine, at, theirs, from_at)

    def early(self, chip, inv, near, a_own, a_other, mine, theirs, part):
        def body(core, chip_of):
            tiles = (a_other, a_own) if core else (a_own, a_other)
            side = augmented(chip[...], inv[...], not core)
            theirs[...] = side
            for k in self.blocks(core, 0, 2):
                block = augmented(near[...] if k else chip[...], inv[...], bool(core))
                mine[self.rows(k), :] = block
                part[self.rows(k), :] = self.add(core, chip_of, tiles, block, [k], side, [0])

        self.on_each_core(body)

    def middle(self, inv, near, far, mine0, theirs0, part0, a_own, a_other, mine, first, part):
        def body(core, chip_of):
            tiles = (a_other, a_own) if core else (a_own, a_other)
            new = self.blocks(1 - core, 1, 2)
            sides = theirs0[...]
            if new:
                side = augmented(far[...], inv[...], not core)
                sides = jnp.concatenate([sides, side], 0)
            for ks in self.groups(core, 2, self.steps + 1):
                rows = self.rows(ks[0] - 2, len(ks))
                block = augmented(near[rows, :], inv[...], bool(core))
                mine[rows, :] = block
                part[rows, :] = self.add(core, chip_of, tiles, block, ks, sides, [0] + new)
            ks = self.blocks(core, 0, 2)
            rows = self.rows(0, len(ks))
            total = part0[rows, :]
            if new:
                total += self.add(core, chip_of, tiles, mine0[rows, :], ks, side, new)
            first[rows, :] = total

        self.on_each_core(body)

    def closed(self, block, total):
        return total[:, self.width :] * block[:, : self.width].astype(F32) - total[:, : self.width]

    def send(self, inv, far, mine0, mine, first, part, a_own, a_other, theirs, *outs):
        def body(core, chip_of):
            tiles = (a_other, a_own) if core else (a_own, a_other)
            have = self.blocks(1 - core, 2, self.steps + 1)
            few = len(have) <= 3
            given = self.rows(have[0] - 2, len(have))
            side = augmented(far[given, :], inv[...], not core)
            theirs[given, :] = side
            for k in range(1, self.steps + 1):
                if k not in self.blocks(core, 1, self.steps + 1):
                    outs[k - 1][...] = jnp.zeros(outs[k - 1].shape, outs[k - 1].dtype)
            for ks in self.groups(core, 1, self.steps + 1):
                parts = [(mine0, first, k) if k == 1 else (mine, part, k - 2) for k in ks]
                block = jnp.concatenate([m[self.rows(at), :] for m, _, at in parts], 0)
                total = jnp.concatenate([p[self.rows(at), :] for _, p, at in parts], 0)
                if few:
                    total += self.add(core, chip_of, tiles, block, ks, side, have)
                else:
                    total = self.rest(core, chip_of, tiles, block, ks, theirs, have, total)
                value = self.closed(block, total)
                for n, k in enumerate(ks):
                    out = outs[k - 1]
                    out[...] = value[n * self.chip : (n + 1) * self.chip].astype(out.dtype)

        self.on_each_core(body)

    def rest(self, core, chip_of, tiles, block, ks, theirs, have, total):
        def step(j, total):
            rows = pl.ds(pl.multiple_of((j - 2) * self.chip, self.chip), self.chip)
            side = theirs[rows, :]
            line, plane, _ = self.here()
            here, n = (plane, self.planes) if core else (line, self.lines)
            from_at = origin(here, self.steps + 1 - j, n)
            at = [chip_of(core, k) for k in ks]
            return total + self.term(core, tiles, block, at, side, [from_at])

        return lax.fori_loop(have[0], have[-1] + 1, step, total)

    def keep(self, mine0, first, theirs, a_own, a_other, out):
        def body(core, chip_of):
            tiles = (a_other, a_own) if core else (a_own, a_other)
            block, total = mine0[self.rows(0), :], first[self.rows(0), :]
            have = self.blocks(1 - core, 2, self.steps + 1)
            if len(have) <= 3:
                side = theirs[self.rows(have[0] - 2, len(have)), :]
                total += self.add(core, chip_of, tiles, block, [0], side, have)
            else:
                total = self.rest(core, chip_of, tiles, block, [0], theirs, have, total)
            out[...] = self.closed(block, total)

        self.on_each_core(body)

    def total(self, *refs):
        inv, terms, (keep, send) = refs[0], refs[1:-2], refs[-2:]
        core = self.here()[2]
        mine = pl.ds(pl.multiple_of(core * self.pts, self.pts), self.pts)
        other = pl.ds(pl.multiple_of((1 - core) * self.pts, self.pts), self.pts)
        for ref, rows in ((keep, mine), (send, other)):
            acc = terms[0][rows, :].astype(F32)
            for term in terms[1:]:
                acc += term[rows, :].astype(F32)
            ref[...] = -acc * inv[...]


def solution(mesh):
    rows, lines = mesh.shape["row"], mesh.shape["col"]
    planes = rows // 2
    steps = max(lines, planes) - 1

    def permute(value, target):
        pairs = []
        for r in range(rows):
            for c in range(lines):
                tr, tc = target(r, c)
                pairs.append((r * lines + c, tr * lines + tc))
        return lax.ppermute(value, AXES, pairs)

    def swap(value):
        return permute(value, lambda r, c: (r ^ 1, c))

    def exchange(value, k):
        distance = steps + 1 - k

        def target(r, c):
            if r % 2:
                return r, partner(c, (distance - 1) % (lines - 1) + 1, lines)
            return 2 * partner(r // 2, (distance - 1) % (planes - 1) + 1, planes), c

        return permute(value, target)

    def local_part(points, abar, inv_scale):
        pts, width = points.shape
        lay = Layout(lines, planes, pts, width)
        chip_rows = lay.chip
        core = lax.axis_index("row") % 2
        inv = inv_scale[None, :]
        grant = pltpu.CompilerParams(vmem_limit_bytes=(6 + steps) * 2**20)

        def call(body, outs, *args):
            return pl.pallas_call(
                body,
                out_shape=[jax.ShapeDtypeStruct(s, t) for s, t in outs],
                in_specs=[VMEM] * len(args),
                out_specs=[VMEM] * len(outs),
                compiler_params=grant,
            )(*args)

        other = swap(points)
        abar_other = swap(abar)
        chip = lax.dynamic_update_slice(
            jnp.zeros((chip_rows, width), points.dtype), points, (core * pts, 0)
        )
        chip = lax.dynamic_update_slice(chip, other, ((1 - core) * pts, 0))
        near = []
        for k in range(1, steps + 1):
            near.append(exchange(chip, k))
        count, wide = abar.shape[0], abar.shape[1] * abar.shape[2]
        cells = [a.reshape(count * wide, abar.shape[3]) for a in (abar, abar_other)]
        if count <= 8 * pts:
            deep = 128
            tiles = pl.pallas_call(
                lambda *refs: relayout(wide, deep, *refs),
                out_shape=[jax.ShapeDtypeStruct((count, wide * width), F32)] * 2,
                in_specs=[VMEM] * 2,
                out_specs=[VMEM] * 2,
                scratch_shapes=[pltpu.VMEM((2, deep * wide, width), F32)],
                compiler_params=grant,
                name="relayout",
            )(*cells)
        else:
            tiles = [a.reshape(count, wide * width).astype(F32) for a in cells]
        far1 = swap(near[0])
        after = jnp.concatenate(near[1:], 0)
        far2 = swap(after)
        deep = 2 * width
        mine0, theirs0, part0 = call(
            lay.early,
            [((2 * chip_rows, deep), BF16), ((chip_rows, deep), BF16), ((2 * chip_rows, deep), F32)],
            chip,
            inv,
            near[0],
            *tiles,
        )
        rest_rows = (steps - 1) * chip_rows
        mine, first, part = call(
            lay.middle,
            [
                ((rest_rows, deep), BF16),
                ((2 * chip_rows, deep), F32),
                ((rest_rows, deep), F32),
            ],
            inv,
            after,
            far1,
            mine0,
            theirs0,
            part0,
            *tiles,
        )
        theirs, *outs = call(
            lay.send,
            [((rest_rows, deep), BF16)] + [((chip_rows, width), BF16)] * steps,
            inv,
            far2,
            mine0,
            mine,
            first,
            part,
            *tiles,
        )
        got = []
        for k in range(1, steps + 1):
            got.append(exchange(outs[k - 1], k))
        (out,) = call(lay.keep, [((chip_rows, width), F32)], mine0, first, theirs, *tiles)
        keep, send = call(lay.total, [((pts, width), F32)] * 2, inv, out, *got)
        return keep + swap(send)

    placed = (P(("row", "col"), None), P("row", None, "col", None), P())
    return jax.shard_map(
        local_part, mesh=mesh, in_specs=placed, out_specs=P(("row", "col"), None), check_vma=False
    )
```

```python
import jax
import jax.numpy as jnp
from jax import lax
from jax.experimental import pallas as pl
from jax.experimental.pallas import tpu as pltpu
from jax.sharding import PartitionSpec as P


F32, BF16 = jnp.float32, jnp.bfloat16
AXES = ("row", "col")
VMEM = pl.BlockSpec(memory_space=pltpu.VMEM)
OVER_LAST, OVER_FIRST, PLAIN = ((1,), (1,)), ((0,), (0,)), ((1,), (0,))


def partner(i, distance, n):
    return i ^ distance if n & (n - 1) == 0 else (i + distance) % n


def origin(i, distance, n):
    return i ^ distance if n & (n - 1) == 0 else (i + n - distance) % n


def dot(a, b, over):
    return lax.dot_general(a, b, (over, ((), ())), preferred_element_type=F32)


def augmented(raw, inv, first):
    s = (raw.astype(F32) * inv).astype(BF16)
    wide = s.astype(F32)
    rest = -0.5 * jnp.sum(wide * wide, axis=1, keepdims=True)
    lane = lax.broadcasted_iota(jnp.int32, s.shape, 1)
    at, ones = (0, 3) if first else (3, 0)
    tail = jnp.where((lane >= ones) & (lane < ones + 3), 1.0, 0.0)
    for n in range(3):
        tail = jnp.where(lane == at + n, rest, tail)
        rest = rest - rest.astype(BF16).astype(F32)
    return jnp.concatenate([s, tail.astype(BF16)], 1)


def relayout(wide, deep, own, other, own_out, other_out, spare):
    width = own.shape[1]
    at = 0
    for ref, out in ((own, own_out), (other, other_out)):
        for start in range(0, out.shape[0], deep):
            spare[at] = ref[start * wide : (start + deep) * wide, :].astype(F32)
            for a in range(wide):
                rows = spare[at, pl.ds(a, deep, stride=wide), :]
                out[start : start + deep, a * width : (a + 1) * width] = rows
            at = 1 - at


class Layout:
    def __init__(self, lines, planes, pts, width):
        self.lines, self.planes, self.pts, self.width = lines, planes, pts, width
        self.steps = max(lines, planes) - 1
        self.chip = 2 * pts

    def here(self):
        row = lax.axis_index("row")
        return lax.axis_index("col"), lax.div(row, 2), lax.rem(row, 2)

    def rows(self, k, n=1):
        return pl.ds(k * self.chip, n * self.chip)

    def blocks(self, side, lo, hi):
        n = (self.planes, self.lines)[side]
        return [k for k in range(lo, hi) if k == 0 or self.steps + 1 - k < n]

    def groups(self, side, lo, hi):
        have = self.blocks(side, lo, hi)
        return [have[i : i + 3] for i in range(0, len(have), 3)]

    def piece(self, tiles, line, plane):
        at = pl.ds(pl.multiple_of(line * self.pts, self.pts), self.pts)
        cols = pl.ds(pl.multiple_of(plane * self.chip, self.chip), self.chip)
        return jnp.concatenate([tile[at, cols] for tile in tiles], 0).astype(F32)

    def term(self, core, tiles, mine, at, theirs, theirs_at):
        if not core and len(at) > 1 and len(theirs_at) > 1:
            parts = []
            for n, j in enumerate(theirs_at):
                rows = theirs[n * self.chip : (n + 1) * self.chip]
                parts.append(self.term(core, tiles, mine, at, rows, [j]))
            return sum(parts[1:], parts[0])
        ones = jnp.ones((theirs.shape[0], self.width), BF16)
        side = jnp.concatenate([theirs[:, : self.width], ones], 1)
        if core:
            e = jnp.exp(dot(mine, theirs, OVER_LAST))
            rows = [[self.piece(tiles, k, j) for j in theirs_at] for k in at]
        else:
            e = jnp.exp(dot(theirs, mine, OVER_LAST))
            rows = [[self.piece(tiles, j, k) for k in at] for j in theirs_at]
        a = jnp.concatenate([jnp.concatenate(row, 1) for row in rows], 0)
        return dot((a * e).astype(BF16), side, PLAIN if core else OVER_FIRST)

    def on_each_core(self, body):
        line, plane, core = self.here()
        for c in (0, 1):

            def chip_of(side, k, line=line, plane=plane):
                here, n = ((plane, self.planes), (line, self.lines))[side]
                return origin(here, self.steps + 1 - k, n) if k else here

            @pl.when(core == c)
            def _(c=c, chip_of=chip_of):
                body(c, chip_of)

    def add(self, core, chip_of, tiles, mine, ks, theirs, js):
        at, from_at = [chip_of(core, k) for k in ks], [chip_of(1 - core, j) for j in js]
        return self.term(core, tiles, mine, at, theirs, from_at)

    def early(self, chip, inv, near, a_own, a_other, mine, theirs, part):
        def body(core, chip_of):
            tiles = (a_other, a_own) if core else (a_own, a_other)
            side = augmented(chip[...], inv[...], not core)
            theirs[...] = side
            for k in self.blocks(core, 0, 2):
                block = augmented(near[...] if k else chip[...], inv[...], bool(core))
                mine[self.rows(k), :] = block
                total = self.add(core, chip_of, tiles, block, [k], side, [0])
                part[self.rows(k), :] = self.closed(block, total)

        self.on_each_core(body)

    def middle(self, inv, near, far, mine0, theirs0, part0, a_own, a_other, mine, first, part):
        def body(core, chip_of):
            tiles = (a_other, a_own) if core else (a_own, a_other)
            new = self.blocks(1 - core, 1, 2)
            sides = theirs0[...]
            if new:
                side = augmented(far[...], inv[...], not core)
                sides = jnp.concatenate([sides, side], 0)
            for ks in self.groups(core, 2, self.steps + 1):
                rows = self.rows(ks[0] - 2, len(ks))
                block = augmented(near[rows, :], inv[...], bool(core))
                mine[rows, :] = block
                total = self.add(core, chip_of, tiles, block, ks, sides, [0] + new)
                part[rows, :] = self.closed(block, total)
            ks = self.blocks(core, 0, 2)
            rows = self.rows(0, len(ks))
            total = part0[rows, :]
            if new:
                block = mine0[rows, :]
                total += self.closed(block, self.add(core, chip_of, tiles, block, ks, side, new))
            first[rows, :] = total

        self.on_each_core(body)

    def closed(self, block, total):
        return total[:, self.width :] * block[:, : self.width].astype(F32) - total[:, : self.width]

    def send(self, inv, far, mine0, mine, first, part, a_own, a_other, theirs, *outs):
        def body(core, chip_of):
            tiles = (a_other, a_own) if core else (a_own, a_other)
            have = self.blocks(1 - core, 2, self.steps + 1)
            few = len(have) <= 3
            given = self.rows(have[0] - 2, len(have))
            side = augmented(far[given, :], inv[...], not core)
            theirs[given, :] = side
            for k in range(1, self.steps + 1):
                if k not in self.blocks(core, 1, self.steps + 1):
                    outs[k - 1][...] = jnp.zeros(outs[k - 1].shape, outs[k - 1].dtype)
            for ks in self.groups(core, 1, self.steps + 1):
                parts = [(mine0, first, k) if k == 1 else (mine, part, k - 2) for k in ks]
                block = jnp.concatenate([m[self.rows(at), :] for m, _, at in parts], 0)
                if few:
                    total = self.add(core, chip_of, tiles, block, ks, side, have)
                else:
                    total = self.rest(core, chip_of, tiles, block, ks, theirs, have)
                value = self.closed(block, total)
                value += jnp.concatenate([p[self.rows(at), :] for _, p, at in parts], 0)
                for n, k in enumerate(ks):
                    out = outs[k - 1]
                    out[...] = value[n * self.chip : (n + 1) * self.chip].astype(out.dtype)

        self.on_each_core(body)

    def rest(self, core, chip_of, tiles, block, ks, theirs, have):
        def step(j, total):
            rows = pl.ds(pl.multiple_of((j - 2) * self.chip, self.chip), self.chip)
            side = theirs[rows, :]
            line, plane, _ = self.here()
            here, n = (plane, self.planes) if core else (line, self.lines)
            from_at = origin(here, self.steps + 1 - j, n)
            at = [chip_of(core, k) for k in ks]
            return total + self.term(core, tiles, block, at, side, [from_at])

        zero = jnp.zeros((block.shape[0], 2 * self.width), F32)
        return lax.fori_loop(have[0], have[-1] + 1, step, zero)

    def keep(self, mine0, first, theirs, a_own, a_other, out):
        def body(core, chip_of):
            tiles = (a_other, a_own) if core else (a_own, a_other)
            block = mine0[self.rows(0), :]
            have = self.blocks(1 - core, 2, self.steps + 1)
            if len(have) <= 3:
                side = theirs[self.rows(have[0] - 2, len(have)), :]
                total = self.add(core, chip_of, tiles, block, [0], side, have)
            else:
                total = self.rest(core, chip_of, tiles, block, [0], theirs, have)
            out[...] = first[self.rows(0), :] + self.closed(block, total)

        self.on_each_core(body)

    def total(self, *refs):
        inv, terms, (keep, send) = refs[0], refs[1:-2], refs[-2:]
        core = self.here()[2]
        mine = pl.ds(pl.multiple_of(core * self.pts, self.pts), self.pts)
        other = pl.ds(pl.multiple_of((1 - core) * self.pts, self.pts), self.pts)
        for ref, rows in ((keep, mine), (send, other)):
            acc = terms[0][rows, :].astype(F32)
            for term in terms[1:]:
                acc += term[rows, :].astype(F32)
            ref[...] = -acc * inv[...]


def solution(mesh):
    rows, lines = mesh.shape["row"], mesh.shape["col"]
    planes = rows // 2
    steps = max(lines, planes) - 1

    def permute(value, target):
        pairs = []
        for r in range(rows):
            for c in range(lines):
                tr, tc = target(r, c)
                pairs.append((r * lines + c, tr * lines + tc))
        return lax.ppermute(value, AXES, pairs)

    def swap(value):
        return permute(value, lambda r, c: (r ^ 1, c))

    def exchange(value, k, to):
        distance = steps + 1 - k

        def target(r, c):
            if r % 2:
                return r, to(c, (distance - 1) % (lines - 1) + 1, lines)
            return 2 * to(r // 2, (distance - 1) % (planes - 1) + 1, planes), c

        return permute(value, target)

    def local_part(points, abar, inv_scale):
        pts, width = points.shape
        lay = Layout(lines, planes, pts, width)
        chip_rows = lay.chip
        core = lax.axis_index("row") % 2
        inv = inv_scale[None, :]
        grant = pltpu.CompilerParams(vmem_limit_bytes=(6 + steps) * 2**20)

        def call(body, outs, *args):
            return pl.pallas_call(
                body,
                out_shape=[jax.ShapeDtypeStruct(s, t) for s, t in outs],
                in_specs=[VMEM] * len(args),
                out_specs=[VMEM] * len(outs),
                compiler_params=grant,
            )(*args)

        other = swap(points)
        abar_other = swap(abar)
        chip = lax.dynamic_update_slice(
            jnp.zeros((chip_rows, width), points.dtype), points, (core * pts, 0)
        )
        chip = lax.dynamic_update_slice(chip, other, ((1 - core) * pts, 0))
        near = []
        for k in range(1, steps + 1):
            near.append(exchange(chip, k, partner))
        count, wide = abar.shape[0], abar.shape[1] * abar.shape[2]
        cells = [a.reshape(count * wide, abar.shape[3]) for a in (abar, abar_other)]
        if count <= 8 * pts:
            deep = 128
            tiles = pl.pallas_call(
                lambda *refs: relayout(wide, deep, *refs),
                out_shape=[jax.ShapeDtypeStruct((count, wide * width), F32)] * 2,
                in_specs=[VMEM] * 2,
                out_specs=[VMEM] * 2,
                scratch_shapes=[pltpu.VMEM((2, deep * wide, width), F32)],
                compiler_params=grant,
                name="relayout",
            )(*cells)
        else:
            tiles = [a.reshape(count, wide * width) for a in cells]
        far1 = swap(near[0])
        after = jnp.concatenate(near[1:], 0)
        far2 = swap(after)
        deep = 2 * width
        mine0, theirs0, part0 = call(
            lay.early,
            [((2 * chip_rows, deep), BF16), ((chip_rows, deep), BF16), ((2 * chip_rows, width), F32)],
            chip,
            inv,
            near[0],
            *tiles,
        )
        rest_rows = (steps - 1) * chip_rows
        mine, first, part = call(
            lay.middle,
            [
                ((rest_rows, deep), BF16),
                ((2 * chip_rows, width), F32),
                ((rest_rows, width), F32),
            ],
            inv,
            after,
            far1,
            mine0,
            theirs0,
            part0,
            *tiles,
        )
        theirs, *outs = call(
            lay.send,
            [((rest_rows, deep), BF16)] + [((chip_rows, width), BF16)] * steps,
            inv,
            far2,
            mine0,
            mine,
            first,
            part,
            *tiles,
        )
        got = []
        for k in range(1, steps + 1):
            got.append(exchange(outs[k - 1], k, origin))
        (out,) = call(lay.keep, [((chip_rows, width), F32)], mine0, first, theirs, *tiles)
        keep, send = call(lay.total, [((pts, width), F32)] * 2, inv, out, *got)
        return keep + swap(send)

    placed = (P(("row", "col"), None), P("row", None, "col", None), P())
    return jax.shard_map(
        local_part, mesh=mesh, in_specs=placed, out_specs=P(("row", "col"), None), check_vma=False
    )
```

```python
import jax
import jax.numpy as jnp
from jax import lax
from jax.experimental import pallas as pl
from jax.experimental.pallas import tpu as pltpu
from jax.sharding import PartitionSpec as P


F32, BF16 = jnp.float32, jnp.bfloat16
AXES = ("row", "col")
VMEM = pl.BlockSpec(memory_space=pltpu.VMEM)
OVER_LAST, OVER_FIRST, PLAIN = ((1,), (1,)), ((0,), (0,)), ((1,), (0,))


def partner(i, distance, n):
    return i ^ distance if n & (n - 1) == 0 else (i + distance) % n


def origin(i, distance, n):
    return i ^ distance if n & (n - 1) == 0 else lax.rem(i + n - distance, n)


def dot(a, b, over):
    return lax.dot_general(a, b, (over, ((), ())), preferred_element_type=F32)


def augmented(raw, inv, first):
    s = (raw.astype(F32) * inv).astype(BF16)
    wide = s.astype(F32)
    rest = -0.5 * jnp.sum(wide * wide, axis=1, keepdims=True)
    lane = lax.broadcasted_iota(jnp.int32, s.shape, 1)
    at, ones = (0, 3) if first else (3, 0)
    tail = jnp.where((lane >= ones) & (lane < ones + 3), 1.0, 0.0)
    for n in range(3):
        tail = jnp.where(lane == at + n, rest, tail)
        rest = rest - rest.astype(BF16).astype(F32)
    return jnp.concatenate([s, tail.astype(BF16)], 1)


def relayout(wide, deep, own, other, own_out, other_out, spare):
    width = own.shape[1]
    at = 0
    for ref, out in ((own, own_out), (other, other_out)):
        for start in range(0, out.shape[0], deep):
            spare[at] = ref[start * wide : (start + deep) * wide, :].astype(F32)
            for a in range(wide):
                rows = spare[at, pl.ds(a, deep, stride=wide), :]
                out[start : start + deep, a * width : (a + 1) * width] = rows
            at = 1 - at


class Layout:
    def __init__(self, lines, planes, pts, width):
        self.lines, self.planes, self.pts, self.width = lines, planes, pts, width
        self.steps = max(lines, planes) - 1
        self.chip = 2 * pts

    def here(self):
        row = lax.axis_index("row")
        return lax.axis_index("col"), lax.div(row, 2), lax.rem(row, 2)

    def rows(self, k, n=1):
        return pl.ds(k * self.chip, n * self.chip)

    def blocks(self, side, lo, hi):
        n = (self.planes, self.lines)[side]
        return [k for k in range(lo, hi) if k == 0 or self.steps + 1 - k < n]

    def groups(self, side, lo, hi):
        have = self.blocks(side, lo, hi)
        return [have[i : i + 3] for i in range(0, len(have), 3)]

    def piece(self, tiles, line, plane):
        at = pl.ds(pl.multiple_of(line * self.pts, self.pts), self.pts)
        cols = pl.ds(pl.multiple_of(plane * self.chip, self.chip), self.chip)
        return jnp.concatenate([tile[at, cols] for tile in tiles], 0)

    def term(self, core, tiles, mine, at, theirs, theirs_at):
        if not core and len(at) > 1 and len(theirs_at) > 1:
            parts = []
            for n, j in enumerate(theirs_at):
                rows = theirs[n * self.chip : (n + 1) * self.chip]
                parts.append(self.term(core, tiles, mine, at, rows, [j]))
            return sum(parts[1:], parts[0])
        ones = jnp.ones((theirs.shape[0], self.width), BF16)
        side = jnp.concatenate([theirs[:, : self.width], ones], 1)
        if core:
            e = jnp.exp(dot(mine, theirs, OVER_LAST))
            rows = [[self.piece(tiles, k, j) for j in theirs_at] for k in at]
        else:
            e = jnp.exp(dot(theirs, mine, OVER_LAST))
            rows = [[self.piece(tiles, j, k) for k in at] for j in theirs_at]
        a = jnp.concatenate([jnp.concatenate(row, 1) for row in rows], 0)
        return dot((a * e).astype(BF16), side, PLAIN if core else OVER_FIRST)

    def on_each_core(self, body):
        line, plane, core = self.here()
        for c in (0, 1):

            def chip_of(side, k, line=line, plane=plane):
                here, n = ((plane, self.planes), (line, self.lines))[side]
                return origin(here, self.steps + 1 - k, n) if k else here

            @pl.when(core == c)
            def _(c=c, chip_of=chip_of):
                body(c, chip_of)

    def add(self, core, chip_of, tiles, mine, ks, theirs, js):
        at, from_at = [chip_of(core, k) for k in ks], [chip_of(1 - core, j) for j in js]
        return self.term(core, tiles, mine, at, theirs, from_at)

    def early(self, chip, inv, near, a_own, a_other, mine, theirs, part):
        def body(core, chip_of):
            tiles = (a_other, a_own) if core else (a_own, a_other)
            side = augmented(chip[...], inv[...], not core)
            theirs[...] = side
            for k in self.blocks(core, 0, 2):
                block = augmented(near[...] if k else chip[...], inv[...], bool(core))
                mine[self.rows(k), :] = block
                part[self.rows(k), :] = self.add(core, chip_of, tiles, block, [k], side, [0])

        self.on_each_core(body)

    def middle(self, inv, near, far, mine0, theirs0, part0, a_own, a_other, mine, first, part):
        def body(core, chip_of):
            tiles = (a_other, a_own) if core else (a_own, a_other)
            new = self.blocks(1 - core, 1, 2)
            sides = theirs0[...]
            if new:
                side = augmented(far[...], inv[...], not core)
                sides = jnp.concatenate([sides, side], 0)
            for ks in self.groups(core, 2, self.steps + 1):
                rows = self.rows(ks[0] - 2, len(ks))
                block = augmented(near[rows, :], inv[...], bool(core))
                mine[rows, :] = block
                part[rows, :] = self.add(core, chip_of, tiles, block, ks, sides, [0] + new)
            ks = self.blocks(core, 0, 2)
            rows = self.rows(0, len(ks))
            total = part0[rows, :]
            if new:
                total += self.add(core, chip_of, tiles, mine0[rows, :], ks, side, new)
            first[rows, :] = total

        self.on_each_core(body)

    def closed(self, block, total):
        return total[:, self.width :] * block[:, : self.width].astype(F32) - total[:, : self.width]

    def send(self, inv, far, mine0, mine, first, part, a_own, a_other, *outs):
        def body(core, chip_of):
            tiles = (a_other, a_own) if core else (a_own, a_other)
            have = self.blocks(1 - core, 2, self.steps + 1)
            few = self.steps <= 4
            theirs = None if few else outs[-1]
            given = self.rows(have[0] - 2, len(have))
            side = augmented(far[given, :], inv[...], not core)
            if not few:
                theirs[given, :] = side
            for k in range(1, self.steps + 1):
                if k not in self.blocks(core, 1, self.steps + 1):
                    outs[k - 1][...] = jnp.zeros(outs[k - 1].shape, outs[k - 1].dtype)
            for ks in self.groups(core, 1, self.steps + 1):
                parts = [(mine0, first, k) if k == 1 else (mine, part, k - 2) for k in ks]
                block = jnp.concatenate([m[self.rows(at), :] for m, _, at in parts], 0)
                total = jnp.concatenate([p[self.rows(at), :] for _, p, at in parts], 0)
                if few:
                    total += self.add(core, chip_of, tiles, block, ks, side, have)
                else:
                    total = self.rest(core, chip_of, tiles, block, ks, theirs, have, total)
                value = self.closed(block, total)
                for n, k in enumerate(ks):
                    out = outs[k - 1]
                    out[...] = value[n * self.chip : (n + 1) * self.chip].astype(out.dtype)

        self.on_each_core(body)

    def rest(self, core, chip_of, tiles, block, ks, theirs, have, total):
        def step(j, total):
            rows = pl.ds(pl.multiple_of((j - 2) * self.chip, self.chip), self.chip)
            side = theirs[rows, :]
            line, plane, _ = self.here()
            here, n = (plane, self.planes) if core else (line, self.lines)
            from_at = origin(here, self.steps + 1 - j, n)
            at = [chip_of(core, k) for k in ks]
            return total + self.term(core, tiles, block, at, side, [from_at])

        return lax.fori_loop(have[0], have[-1] + 1, step, total)

    def keep(self, inv, mine0, first, theirs, a_own, a_other, out):
        def body(core, chip_of):
            tiles = (a_other, a_own) if core else (a_own, a_other)
            block, total = mine0[self.rows(0), :], first[self.rows(0), :]
            have = self.blocks(1 - core, 2, self.steps + 1)
            if self.steps <= 4:
                raw = theirs[self.rows(have[0] - 2, len(have)), :]
                side = augmented(raw, inv[...], not core)
                total += self.add(core, chip_of, tiles, block, [0], side, have)
            else:
                total = self.rest(core, chip_of, tiles, block, [0], theirs, have, total)
            out[...] = self.closed(block, total)

        self.on_each_core(body)

    def total(self, *refs):
        inv, terms, (keep, send) = refs[0], refs[1:-2], refs[-2:]
        core = self.here()[2]
        mine = pl.ds(pl.multiple_of(core * self.pts, self.pts), self.pts)
        other = pl.ds(pl.multiple_of((1 - core) * self.pts, self.pts), self.pts)
        for ref, rows in ((keep, mine), (send, other)):
            acc = terms[0][rows, :].astype(F32)
            for term in terms[1:]:
                acc += term[rows, :].astype(F32)
            ref[...] = (-acc * inv[...]).astype(ref.dtype)


def solution(mesh):
    rows, lines = mesh.shape["row"], mesh.shape["col"]
    planes = rows // 2
    steps = max(lines, planes) - 1

    def permute(value, target):
        pairs = []
        for r in range(rows):
            for c in range(lines):
                tr, tc = target(r, c)
                pairs.append((r * lines + c, tr * lines + tc))
        return lax.ppermute(value, AXES, pairs)

    def swap(value):
        return permute(value, lambda r, c: (r ^ 1, c))

    def exchange(value, k):
        distance = steps + 1 - k

        def target(r, c):
            if r % 2:
                return r, partner(c, (distance - 1) % (lines - 1) + 1, lines)
            return 2 * partner(r // 2, (distance - 1) % (planes - 1) + 1, planes), c

        return permute(value, target)

    def local_part(points, abar, inv_scale):
        pts, width = points.shape
        lay = Layout(lines, planes, pts, width)
        chip_rows = lay.chip
        core = lax.axis_index("row") % 2
        inv = inv_scale[None, :]
        grant = pltpu.CompilerParams(vmem_limit_bytes=(6 + steps) * 2**20)

        def call(body, outs, *args):
            return pl.pallas_call(
                body,
                out_shape=[jax.ShapeDtypeStruct(s, t) for s, t in outs],
                in_specs=[VMEM] * len(args),
                out_specs=[VMEM] * len(outs),
                compiler_params=grant,
            )(*args)

        other = swap(points)
        abar_other = swap(abar)
        chip = lax.dynamic_update_slice(
            jnp.zeros((chip_rows, width), points.dtype), points, (core * pts, 0)
        )
        chip = lax.dynamic_update_slice(chip, other, ((1 - core) * pts, 0))
        near = []
        for k in range(1, steps + 1):
            near.append(exchange(chip, k))
        count, wide = abar.shape[0], abar.shape[1] * abar.shape[2]
        cells = [a.reshape(count * wide, abar.shape[3]) for a in (abar, abar_other)]
        if count <= 8 * pts:
            deep = 128
            tiles = pl.pallas_call(
                lambda *refs: relayout(wide, deep, *refs),
                out_shape=[jax.ShapeDtypeStruct((count, wide * width), F32)] * 2,
                in_specs=[VMEM] * 2,
                out_specs=[VMEM] * 2,
                scratch_shapes=[pltpu.VMEM((2, deep * wide, width), F32)],
                compiler_params=grant,
                name="relayout",
            )(*cells)
        else:
            tiles = [a.reshape(count, wide * width).astype(F32) for a in cells]
        far1 = swap(near[0])
        after = jnp.concatenate(near[1:], 0)
        far2 = swap(after)
        deep = 2 * width
        mine0, theirs0, part0 = call(
            lay.early,
            [((2 * chip_rows, deep), BF16), ((chip_rows, deep), BF16), ((2 * chip_rows, deep), F32)],
            chip,
            inv,
            near[0],
            *tiles,
        )
        rest_rows = (steps - 1) * chip_rows
        mine, first, part = call(
            lay.middle,
            [
                ((rest_rows, deep), BF16),
                ((2 * chip_rows, deep), F32),
                ((rest_rows, deep), F32),
            ],
            inv,
            after,
            far1,
            mine0,
            theirs0,
            part0,
            *tiles,
        )
        outs = call(
            lay.send,
            [((chip_rows, width), BF16)] * steps + [((rest_rows, deep), BF16)] * (steps > 4),
            inv,
            far2,
            mine0,
            mine,
            first,
            part,
            *tiles,
        )
        got = []
        for k in range(1, steps + 1):
            got.append(exchange(outs[k - 1], k))
        (out,) = call(lay.keep, [((chip_rows, width), F32)], inv, mine0, first, far2 if steps <= 4 else outs[-1], *tiles)
        keep, send = call(lay.total, [((pts, width), F32), ((pts, width), BF16)], inv, out, *got)
        return keep + swap(send).astype(F32)

    placed = (P(("row", "col"), None), P("row", None, "col", None), P())
    return jax.shard_map(
        local_part, mesh=mesh, in_specs=placed, out_specs=P(("row", "col"), None), check_vma=False
    )
```

```python
import jax
import jax.numpy as jnp
from jax import lax
from jax.experimental import pallas as pl
from jax.experimental.pallas import tpu as pltpu
from jax.sharding import PartitionSpec as P


F32, BF16 = jnp.float32, jnp.bfloat16
AXES = ("row", "col")
VMEM = pl.BlockSpec(memory_space=pltpu.VMEM)
OVER_LAST, OVER_FIRST, PLAIN = ((1,), (1,)), ((0,), (0,)), ((1,), (0,))


def partner(i, distance, n):
    return i ^ distance if n & (n - 1) == 0 else (i + distance) % n


def origin(i, distance, n):
    return i ^ distance if n & (n - 1) == 0 else (i + n - distance) % n


def dot(a, b, over):
    return lax.dot_general(a, b, (over, ((), ())), preferred_element_type=F32)


def augmented(raw, inv, first):
    s = (raw.astype(F32) * inv).astype(BF16)
    wide = s.astype(F32)
    rest = -0.5 * jnp.sum(wide * wide, axis=1, keepdims=True)
    lane = lax.broadcasted_iota(jnp.int32, s.shape, 1)
    at, ones = (0, 3) if first else (3, 0)
    tail = jnp.where((lane >= ones) & (lane < ones + 3), 1.0, 0.0)
    for n in range(3):
        tail = jnp.where(lane == at + n, rest, tail)
        rest = rest - rest.astype(BF16).astype(F32)
    return jnp.concatenate([s, tail.astype(BF16)], 1)


def relayout(wide, deep, own, other, own_out, other_out, spare):
    width = own.shape[1]
    at = 0
    for ref, out in ((own, own_out), (other, other_out)):
        for start in range(0, out.shape[0], deep):
            spare[at] = ref[start * wide : (start + deep) * wide, :].astype(F32)
            for a in range(wide):
                rows = spare[at, pl.ds(a, deep, stride=wide), :]
                out[start : start + deep, a * width : (a + 1) * width] = rows
            at = 1 - at


ORDERS = ((2, 3, 1), (2, 3, 1))


def distance_of(steps, side, k):
    return ORDERS[side][k - 1] if steps == 3 else steps + 1 - k


class Layout:
    def __init__(self, lines, planes, pts, width):
        self.lines, self.planes, self.pts, self.width = lines, planes, pts, width
        self.steps = max(lines, planes) - 1
        self.chip = 2 * pts

    def here(self):
        row = lax.axis_index("row")
        return lax.axis_index("col"), lax.div(row, 2), lax.rem(row, 2)

    def rows(self, k, n=1):
        return pl.ds(k * self.chip, n * self.chip)

    def blocks(self, side, lo, hi):
        n = (self.planes, self.lines)[side]
        return [k for k in range(lo, hi) if k == 0 or distance_of(self.steps, side, k) < n]

    def groups(self, side, lo, hi):
        have = self.blocks(side, lo, hi)
        return [have[i : i + 3] for i in range(0, len(have), 3)]

    def piece(self, tiles, line, plane):
        at = pl.ds(pl.multiple_of(line * self.pts, self.pts), self.pts)
        cols = pl.ds(pl.multiple_of(plane * self.chip, self.chip), self.chip)
        return jnp.concatenate([tile[at, cols] for tile in tiles], 0).astype(F32)

    def term(self, core, tiles, mine, at, theirs, theirs_at):
        if not core and len(at) > 1 and len(theirs_at) > 1:
            parts = []
            for n, j in enumerate(theirs_at):
                rows = theirs[n * self.chip : (n + 1) * self.chip]
                parts.append(self.term(core, tiles, mine, at, rows, [j]))
            return sum(parts[1:], parts[0])
        ones = jnp.ones((theirs.shape[0], self.width), BF16)
        side = jnp.concatenate([theirs[:, : self.width], ones], 1)
        if core:
            e = jnp.exp(dot(mine, theirs, OVER_LAST))
            rows = [[self.piece(tiles, k, j) for j in theirs_at] for k in at]
        else:
            e = jnp.exp(dot(theirs, mine, OVER_LAST))
            rows = [[self.piece(tiles, j, k) for k in at] for j in theirs_at]
        a = jnp.concatenate([jnp.concatenate(row, 1) for row in rows], 0)
        return dot((a * e).astype(BF16), side, PLAIN if core else OVER_FIRST)

    def on_each_core(self, body):
        line, plane, core = self.here()
        for c in (0, 1):

            def chip_of(side, k, line=line, plane=plane):
                here, n = ((plane, self.planes), (line, self.lines))[side]
                return origin(here, distance_of(self.steps, side, k), n) if k else here

            @pl.when(core == c)
            def _(c=c, chip_of=chip_of):
                body(c, chip_of)

    def add(self, core, chip_of, tiles, mine, ks, theirs, js):
        at, from_at = [chip_of(core, k) for k in ks], [chip_of(1 - core, j) for j in js]
        return self.term(core, tiles, mine, at, theirs, from_at)

    def early(self, chip, inv, near, a_own, a_other, mine, theirs, part):
        def body(core, chip_of):
            tiles = (a_other, a_own) if core else (a_own, a_other)
            side = augmented(chip[...], inv[...], not core)
            theirs[...] = side
            for k in self.blocks(core, 0, 2):
                block = augmented(near[...] if k else chip[...], inv[...], bool(core))
                mine[self.rows(k), :] = block
                total = self.add(core, chip_of, tiles, block, [k], side, [0])
                part[self.rows(k), :] = self.closed(block, total)

        self.on_each_core(body)

    def middle(self, inv, near, far, mine0, theirs0, part0, a_own, a_other, mine, first, part):
        def body(core, chip_of):
            tiles = (a_other, a_own) if core else (a_own, a_other)
            new = self.blocks(1 - core, 1, 2)
            sides = theirs0[...]
            if new:
                side = augmented(far[...], inv[...], not core)
                sides = jnp.concatenate([sides, side], 0)
            for ks in self.groups(core, 2, self.steps + 1):
                rows = self.rows(ks[0] - 2, len(ks))
                block = augmented(near[rows, :], inv[...], bool(core))
                mine[rows, :] = block
                total = self.add(core, chip_of, tiles, block, ks, sides, [0] + new)
                part[rows, :] = self.closed(block, total)
            ks = self.blocks(core, 0, 2)
            rows = self.rows(0, len(ks))
            total = part0[rows, :]
            if new:
                block = mine0[rows, :]
                total += self.closed(block, self.add(core, chip_of, tiles, block, ks, side, new))
            first[rows, :] = total

        self.on_each_core(body)

    def closed(self, block, total):
        return total[:, self.width :] * block[:, : self.width].astype(F32) - total[:, : self.width]

    def send(self, inv, far, mine0, mine, first, part, a_own, a_other, theirs, *outs):
        def body(core, chip_of):
            tiles = (a_other, a_own) if core else (a_own, a_other)
            have = self.blocks(1 - core, 2, self.steps + 1)
            few = len(have) <= 3
            given = self.rows(have[0] - 2, len(have))
            side = augmented(far[given, :], inv[...], not core)
            theirs[given, :] = side
            for k in range(1, self.steps + 1):
                if k not in self.blocks(core, 1, self.steps + 1):
                    outs[k - 1][...] = jnp.zeros(outs[k - 1].shape, outs[k - 1].dtype)
            for ks in self.groups(core, 1, self.steps + 1):
                parts = [(mine0, first, k) if k == 1 else (mine, part, k - 2) for k in ks]
                block = jnp.concatenate([m[self.rows(at), :] for m, _, at in parts], 0)
                if few:
                    total = self.add(core, chip_of, tiles, block, ks, side, have)
                else:
                    total = self.rest(core, chip_of, tiles, block, ks, theirs, have)
                value = self.closed(block, total)
                value += jnp.concatenate([p[self.rows(at), :] for _, p, at in parts], 0)
                for n, k in enumerate(ks):
                    out = outs[k - 1]
                    out[...] = value[n * self.chip : (n + 1) * self.chip].astype(out.dtype)

        self.on_each_core(body)

    def rest(self, core, chip_of, tiles, block, ks, theirs, have):
        def step(j, total):
            rows = pl.ds(pl.multiple_of((j - 2) * self.chip, self.chip), self.chip)
            side = theirs[rows, :]
            line, plane, _ = self.here()
            here, n = (plane, self.planes) if core else (line, self.lines)
            from_at = origin(here, self.steps + 1 - j, n)
            at = [chip_of(core, k) for k in ks]
            return total + self.term(core, tiles, block, at, side, [from_at])

        zero = jnp.zeros((block.shape[0], 2 * self.width), F32)
        return lax.fori_loop(have[0], have[-1] + 1, step, zero)

    def keep(self, mine0, first, theirs, a_own, a_other, out):
        def body(core, chip_of):
            tiles = (a_other, a_own) if core else (a_own, a_other)
            block = mine0[self.rows(0), :]
            have = self.blocks(1 - core, 2, self.steps + 1)
            if len(have) <= 3:
                side = theirs[self.rows(have[0] - 2, len(have)), :]
                total = self.add(core, chip_of, tiles, block, [0], side, have)
            else:
                total = self.rest(core, chip_of, tiles, block, [0], theirs, have)
            out[...] = first[self.rows(0), :] + self.closed(block, total)

        self.on_each_core(body)

    def total(self, *refs):
        inv, terms, (keep, send) = refs[0], refs[1:-2], refs[-2:]
        core = self.here()[2]
        mine = pl.ds(pl.multiple_of(core * self.pts, self.pts), self.pts)
        other = pl.ds(pl.multiple_of((1 - core) * self.pts, self.pts), self.pts)
        for ref, rows in ((keep, mine), (send, other)):
            acc = terms[0][rows, :].astype(F32)
            for term in terms[1:]:
                acc += term[rows, :].astype(F32)
            ref[...] = -acc * inv[...]


def solution(mesh):
    rows, lines = mesh.shape["row"], mesh.shape["col"]
    planes = rows // 2
    steps = max(lines, planes) - 1

    def permute(value, target):
        pairs = []
        for r in range(rows):
            for c in range(lines):
                tr, tc = target(r, c)
                pairs.append((r * lines + c, tr * lines + tc))
        return lax.ppermute(value, AXES, pairs)

    def swap(value):
        return permute(value, lambda r, c: (r ^ 1, c))

    def exchange(value, k, to):
        over_row, over_col = (distance_of(steps, side, k) for side in (0, 1))

        def target(r, c):
            if r % 2:
                return r, to(c, (over_col - 1) % (lines - 1) + 1, lines)
            return 2 * to(r // 2, (over_row - 1) % (planes - 1) + 1, planes), c

        return permute(value, target)

    def local_part(points, abar, inv_scale):
        pts, width = points.shape
        lay = Layout(lines, planes, pts, width)
        chip_rows = lay.chip
        core = lax.axis_index("row") % 2
        inv = inv_scale[None, :]
        grant = pltpu.CompilerParams(vmem_limit_bytes=(6 + steps) * 2**20)

        def call(body, outs, *args):
            return pl.pallas_call(
                body,
                out_shape=[jax.ShapeDtypeStruct(s, t) for s, t in outs],
                in_specs=[VMEM] * len(args),
                out_specs=[VMEM] * len(outs),
                compiler_params=grant,
            )(*args)

        other = swap(points)
        abar_other = swap(abar)
        chip = lax.dynamic_update_slice(
            jnp.zeros((chip_rows, width), points.dtype), points, (core * pts, 0)
        )
        chip = lax.dynamic_update_slice(chip, other, ((1 - core) * pts, 0))
        near = []
        for k in range(1, steps + 1):
            near.append(exchange(chip, k, partner))
        count, wide = abar.shape[0], abar.shape[1] * abar.shape[2]
        cells = [a.reshape(count * wide, abar.shape[3]) for a in (abar, abar_other)]
        if count <= 8 * pts:
            deep = 128
            tiles = pl.pallas_call(
                lambda *refs: relayout(wide, deep, *refs),
                out_shape=[jax.ShapeDtypeStruct((count, wide * width), F32)] * 2,
                in_specs=[VMEM] * 2,
                out_specs=[VMEM] * 2,
                scratch_shapes=[pltpu.VMEM((2, deep * wide, width), F32)],
                compiler_params=grant,
                name="relayout",
            )(*cells)
        else:
            tiles = [a.reshape(count, wide * width) for a in cells]
        far1 = swap(near[0])
        after = jnp.concatenate(near[1:], 0)
        far2 = swap(after)
        deep = 2 * width
        mine0, theirs0, part0 = call(
            lay.early,
            [((2 * chip_rows, deep), BF16), ((chip_rows, deep), BF16), ((2 * chip_rows, width), F32)],
            chip,
            inv,
            near[0],
            *tiles,
        )
        rest_rows = (steps - 1) * chip_rows
        mine, first, part = call(
            lay.middle,
            [
                ((rest_rows, deep), BF16),
                ((2 * chip_rows, width), F32),
                ((rest_rows, width), F32),
            ],
            inv,
            after,
            far1,
            mine0,
            theirs0,
            part0,
            *tiles,
        )
        theirs, *outs = call(
            lay.send,
            [((rest_rows, deep), BF16)] + [((chip_rows, width), BF16)] * steps,
            inv,
            far2,
            mine0,
            mine,
            first,
            part,
            *tiles,
        )
        got = []
        for k in range(1, steps + 1):
            got.append(exchange(outs[k - 1], k, origin))
        (out,) = call(lay.keep, [((chip_rows, width), F32)], mine0, first, theirs, *tiles)
        keep, send = call(lay.total, [((pts, width), F32)] * 2, inv, out, *got)
        return keep + swap(send)

    placed = (P(("row", "col"), None), P("row", None, "col", None), P())
    return jax.shard_map(
        local_part, mesh=mesh, in_specs=placed, out_specs=P(("row", "col"), None), check_vma=False
    )
```
